32 devices in a mesh: dp: 8 (over y, x, core), mp: 4 (over z).
Axes of the slice: x: 2, y: 2, z: 4, core: 2. Of those that a mesh axis runs over, the one named last changes fastest.
Arguments:
- tokens: bfloat16 [512, 8192], P('mp', 'dp'), may hold values from -6 to 6
- cotangent: bfloat16 [512, 8192], P('mp', 'dp'), may hold values from -1.5 to 1.5
- gate_weight: bfloat16 [8192, 14336], P('dp', 'mp'), may hold values from -0.0625 to 0.0625
- up_weight: bfloat16 [8192, 14336], P('dp', 'mp'), may hold values from -0.0625 to 0.0625
- down_weight: bfloat16 [14336, 8192], P('mp', 'dp'), may hold values from -0.046875 to 0.046875
Outputs:
- output: bfloat16 [512, 8192], P('mp', 'dp')
- grad_input: bfloat16 [512, 8192], P('mp', 'dp')
- grad_gate: bfloat16 [8192, 14336], P('dp', 'mp')
- grad_up: bfloat16 [8192, 14336], P('dp', 'mp')
- grad_down: bfloat16 [14336, 8192], P('mp', 'dp')
The draws below stay inside these ranges and needn't reach their ends.
All inputs are finite; a program needn't handle non-finite values.
Results may differ from the reference program's by a relative error of at most 0.013.
Values may be sent and summed in bfloat16 or wider, within the bound.
A program may use at most 128 MiB of HBM per device.

```python
import jax
import jax.numpy as jnp
from jax import lax

D = 8192
FF = 14336
TOKENS = 512


def shard_levels(rng, extent, split, least, high):
    def one(position, blocks):
        steps = jax.random.uniform(jax.random.fold_in(jax.random.fold_in(rng, 6), position), (blocks,), jnp.float32, least / len(split), high / len(split))
        return jnp.repeat(jnp.exp(steps), extent[position] // blocks).reshape((-1,) + (1,) * (len(extent) - position - 1))

    factor_of = one(*split[0])
    for cut in split[1:]:
        factor_of = factor_of * one(*cut)
    return factor_of


def centred(key, shape, width, reach, shards=(), dtype=jnp.bfloat16):
    level = shard_levels(key, shape, shards, -0.22, 0.18) if shards else 1.0
    drawn = jax.random.normal(key, shape, jnp.float32) * width * level
    return jnp.minimum(jnp.maximum(drawn, -reach), reach).astype(dtype)


def setup_inputs(seed: int = 0) -> dict:
    splits = jax.random.split(jax.random.key(seed), 6)
    return {
        "tokens": centred(splits[0], (TOKENS, D), 1.0, 6.0, ((0, 4), (1, 8))),
        "cotangent": centred(splits[1], (TOKENS, D), 0.25, 1.5, ((0, 4), (1, 8))),
        "gate_weight": centred(splits[2], (D, FF), D ** -0.5, 0.0625, ((0, 8), (1, 4))),
        "up_weight": centred(splits[3], (D, FF), D ** -0.5, 0.0625, ((0, 8), (1, 4))),
        "down_weight": centred(splits[4], (FF, D), FF ** -0.5, 0.046875, ((0, 4), (1, 8))),
    }


def contract(left, right, left_dim, right_dim):
    return lax.dot_general(left, right, (((left_dim,), (right_dim,)), ((), ())), preferred_element_type=jnp.float32)


def reference(tokens, cotangent, gate_weight, up_weight, down_weight):
    gate = jnp.dot(tokens, gate_weight, preferred_element_type=jnp.float32)
    up = jnp.dot(tokens, up_weight, preferred_element_type=jnp.float32)
    sig = jax.nn.sigmoid(gate)
    hidden = (gate * sig * up).astype(jnp.bfloat16)
    output = jnp.dot(hidden, down_weight, preferred_element_type=jnp.float32).astype(jnp.bfloat16)
    d_hidden = contract(cotangent, down_weight, 1, 1)
    d_gate = (d_hidden * up * sig * (1.0 + gate * (1.0 - sig))).astype(jnp.bfloat16)
    d_up = (d_hidden * gate * sig).astype(jnp.bfloat16)
    grad_down = contract(hidden, cotangent, 0, 0).astype(jnp.bfloat16)
    grad_gate = contract(tokens, d_gate, 0, 0).astype(jnp.bfloat16)
    grad_up = contract(tokens, d_up, 0, 0).astype(jnp.bfloat16)
    grad_input = (contract(d_gate, gate_weight, 1, 1) + contract(d_up, up_weight, 1, 1)).astype(jnp.bfloat16)
    return (output, grad_input, grad_gate, grad_up, grad_down)
```

```python
import jax
import jax.numpy as jnp
from jax import lax
from jax.sharding import PartitionSpec as P

F32, BF16 = jnp.float32, jnp.bfloat16


def contract(left, right, left_dim, right_dim):
    return lax.dot_general(
        left, right, (((left_dim,), (right_dim,)), ((), ())), preferred_element_type=F32
    )


def orders(bits):
    return [0] + list(range(1, bits)), [0] + list(range(bits - 1, 0, -1))


def partners(n, bits, step):
    both = orders(bits)
    return [(i, i ^ (1 << both[i & 1][step])) for i in range(n)]


def localize(x, bits, index, inverse=False):
    even, odd = orders(bits)
    rows, tail = x.shape[0] >> bits, x.shape[1:]
    x = x.reshape((2,) * bits + (rows,) + tail)

    def bit(k):
        return (index >> k) & 1

    def flips(half, order):
        for axis, k in enumerate(order[1:]):
            half = jnp.where(bit(k) == 1, jnp.flip(half, axis), half)
        return half

    rest = [bits, *range(bits + 1, bits + 1 + len(tail))]
    if not inverse:
        parts = []
        for core, order in enumerate((even, odd)):
            moved = x.transpose([bits - 1 - k for k in order] + rest)[core]
            parts.append(flips(moved, order))
        low = jnp.where(bit(0) == 1, parts[1], parts[0])
        high = jnp.where(bit(0) == 1, parts[0], parts[1])
        out = jnp.stack([low, high])
    else:
        low = jnp.where(bit(0) == 1, x[1], x[0])
        high = jnp.where(bit(0) == 1, x[0], x[1])
        parts = []
        for half, order in ((low, even), (high, odd)):
            half = flips(half, order)
            at = {k: a for a, k in enumerate(order[1:])}
            parts.append(
                half.transpose(
                    [at[k] for k in range(bits - 1, 0, -1)]
                    + [bits - 1 + j for j in range(1 + len(tail))]
                )
            )
        out = jnp.stack(parts, axis=bits - 1)
    return out.reshape((-1,) + tail)


def ring(n, shift):
    return [(i, (i + shift) % n) for i in range(n)]


def gather_mp(x, n):
    blocks = [None] * n
    blocks[0] = x
    if n == 1:
        return blocks
    up = down = x
    for s in range(1, (n - 1) // 2 + 1):
        up = lax.ppermute(up, "mp", ring(n, 1))
        down = lax.ppermute(down, "mp", ring(n, -1))
        blocks[n - s], blocks[s] = up, down
    if n % 2 == 0:
        half = x.shape[0] // 2
        low = lax.ppermute(up[:half], "mp", ring(n, 1))
        high = lax.ppermute(down[half:], "mp", ring(n, -1))
        blocks[n // 2] = jnp.concatenate([low, high])
    return blocks


def scatter_mp(blocks, n):
    if n == 1:
        return blocks[0].astype(BF16)
    far = (n - 1) // 2
    up = down = None
    if n % 2 == 0:
        piece = blocks[n // 2].astype(BF16)
        half = piece.shape[0] // 2
        up = lax.ppermute(piece[:half], "mp", ring(n, 1))
        down = lax.ppermute(piece[half:], "mp", ring(n, -1))
        pad_up = lambda a, r: jnp.concatenate([a[:half] + r.astype(F32), a[half:]])
        pad_down = lambda a, r: jnp.concatenate([a[:half], a[half:] + r.astype(F32)])
    for s in range(far, 0, -1):
        a, b = blocks[s].astype(F32), blocks[n - s].astype(F32)
        if up is not None:
            if s == far and n % 2 == 0:
                a, b = pad_up(a, up), pad_down(b, down)
            else:
                a, b = a + up.astype(F32), b + down.astype(F32)
        up = lax.ppermute(a.astype(BF16), "mp", ring(n, 1))
        down = lax.ppermute(b.astype(BF16), "mp", ring(n, -1))
    own = blocks[0].astype(F32)
    if far == 0:
        return jnp.concatenate([own[:half] + up, own[half:] + down]).astype(BF16)
    return (own + up.astype(F32) + down.astype(F32)).astype(BF16)


def per_device(tokens, cotangent, gate_weight, up_weight, down_weight):
    n_dp, n_mp = lax.axis_size("dp"), lax.axis_size("mp")
    bits = n_dp.bit_length() - 1
    assert 1 << bits == n_dp and bits >= 1
    index = lax.axis_index("dp")
    width = tokens.shape[1]

    def assemble(x):
        blocks = gather_mp(localize(x, bits, index), n_mp)
        return jnp.stack([b.reshape(n_dp, -1, width) for b in blocks], axis=1).reshape(-1, width)

    def swap(x, step):
        return lax.ppermute(x, "dp", partners(n_dp, bits, step))

    def reduce_dp(rows, dot):
        half = rows.shape[0] // 2
        got = swap(dot(rows[half:]).astype(BF16), 0)
        kept = lax.optimization_barrier(dot(rows[:half]))
        for step in range(1, bits):
            total = kept + got.astype(F32)
            half = half // 2
            got = swap(total[half:].astype(BF16), step)
            kept = total[:half]
        return kept + got.astype(F32)

    def gather_dp(x):
        for step in range(bits - 1, -1, -1):
            x = jnp.concatenate([x, swap(x, step)])
        return x

    def finish(partial):
        partial = partial.astype(BF16).reshape(n_dp, n_mp, -1, width)
        blocks = [partial[:, k].reshape(-1, width) for k in range(n_mp)]
        return localize(scatter_mp(blocks, n_mp), bits, index, inverse=True)

    all_tokens = assemble(tokens)
    gate = reduce_dp(all_tokens, lambda r: contract(r, gate_weight, 1, 0))
    up = reduce_dp(all_tokens, lambda r: contract(r, up_weight, 1, 0))
    all_cotangent = assemble(cotangent)
    d_hidden = reduce_dp(all_cotangent, lambda r: contract(r, down_weight, 1, 1))
    sig = jax.nn.sigmoid(gate)
    hidden = (gate * sig * up).astype(BF16)
    all_hidden = gather_dp(hidden)
    d_gate = (d_hidden * up * sig * (1.0 + gate * (1.0 - sig))).astype(BF16)
    d_up = (d_hidden * gate * sig).astype(BF16)
    all_d_gate, all_d_up = gather_dp(d_gate), gather_dp(d_up)

    output = finish(contract(all_hidden, down_weight, 1, 0))
    grad_input = finish(
        contract(all_d_gate, gate_weight, 1, 1) + contract(all_d_up, up_weight, 1, 1)
    )
    turned = all_tokens.T
    grad_down = contract(all_hidden, all_cotangent, 0, 0).astype(BF16)
    grad_gate = contract(turned, all_d_gate, 1, 0).astype(BF16)
    grad_up = contract(turned, all_d_up, 1, 0).astype(BF16)
    return (output, grad_input, grad_gate, grad_up, grad_down)


def solution(mesh):
    placed = (P("mp", "dp"), P("mp", "dp"), P("dp", "mp"), P("dp", "mp"), P("mp", "dp"))
    return jax.shard_map(
        per_device,
        mesh=mesh,
        in_specs=placed,
        out_specs=(P("mp", "dp"), P("mp", "dp"), P("dp", "mp"), P("dp", "mp"), P("mp", "dp")),
        check_vma=False,
    )
```

```python
import jax
import jax.numpy as jnp
from jax import lax
from jax.sharding import PartitionSpec as P

F32, BF16 = jnp.float32, jnp.bfloat16


def contract(left, right, left_dim, right_dim):
    return lax.dot_general(
        left, right, (((left_dim,), (right_dim,)), ((), ())), preferred_element_type=F32
    )


def orders(bits):
    return [0] + list(range(1, bits)), [0] + list(range(bits - 1, 0, -1))


def partners(n, bits, step):
    both = orders(bits)
    return [(i, i ^ (1 << both[i & 1][step])) for i in range(n)]


def localize(x, bits, index, inverse=False):
    even, odd = orders(bits)
    rows, tail = x.shape[0] >> bits, x.shape[1:]
    x = x.reshape((2,) * bits + (rows,) + tail)

    def bit(k):
        return (index >> k) & 1

    def flips(half, order):
        for axis, k in enumerate(order[1:]):
            half = jnp.where(bit(k) == 1, jnp.flip(half, axis), half)
        return half

    rest = [bits, *range(bits + 1, bits + 1 + len(tail))]
    if not inverse:
        parts = []
        for core, order in enumerate((even, odd)):
            moved = x.transpose([bits - 1 - k for k in order] + rest)[core]
            parts.append(flips(moved, order))
        low = jnp.where(bit(0) == 1, parts[1], parts[0])
        high = jnp.where(bit(0) == 1, parts[0], parts[1])
        out = jnp.stack([low, high])
    else:
        low = jnp.where(bit(0) == 1, x[1], x[0])
        high = jnp.where(bit(0) == 1, x[0], x[1])
        parts = []
        for half, order in ((low, even), (high, odd)):
            half = flips(half, order)
            at = {k: a for a, k in enumerate(order[1:])}
            parts.append(
                half.transpose(
                    [at[k] for k in range(bits - 1, 0, -1)]
                    + [bits - 1 + j for j in range(1 + len(tail))]
                )
            )
        out = jnp.stack(parts, axis=bits - 1)
    return out.reshape((-1,) + tail)


def ring(n, shift):
    return [(i, (i + shift) % n) for i in range(n)]


def gather_mp(x, n):
    blocks = [None] * n
    blocks[0] = x
    if n == 1:
        return blocks
    up = down = x
    for s in range(1, (n - 1) // 2 + 1):
        up = lax.ppermute(up, "mp", ring(n, 1))
        down = lax.ppermute(down, "mp", ring(n, -1))
        blocks[n - s], blocks[s] = up, down
    if n % 2 == 0:
        half = x.shape[0] // 2
        low = lax.ppermute(up[:half], "mp", ring(n, 1))
        high = lax.ppermute(down[half:], "mp", ring(n, -1))
        blocks[n // 2] = jnp.concatenate([low, high])
    return blocks


def scatter_mp(blocks, n):
    if n == 1:
        return blocks[0].astype(BF16)
    far = (n - 1) // 2
    up = down = None
    if n % 2 == 0:
        piece = blocks[n // 2].astype(BF16)
        half = piece.shape[0] // 2
        up = lax.ppermute(piece[:half], "mp", ring(n, 1))
        down = lax.ppermute(piece[half:], "mp", ring(n, -1))
        pad_up = lambda a, r: jnp.concatenate([a[:half] + r.astype(F32), a[half:]])
        pad_down = lambda a, r: jnp.concatenate([a[:half], a[half:] + r.astype(F32)])
    for s in range(far, 0, -1):
        a, b = blocks[s].astype(F32), blocks[n - s].astype(F32)
        if up is not None:
            if s == far and n % 2 == 0:
                a, b = pad_up(a, up), pad_down(b, down)
            else:
                a, b = a + up.astype(F32), b + down.astype(F32)
        up = lax.ppermute(a.astype(BF16), "mp", ring(n, 1))
        down = lax.ppermute(b.astype(BF16), "mp", ring(n, -1))
    own = blocks[0].astype(F32)
    if far == 0:
        return jnp.concatenate([own[:half] + up, own[half:] + down]).astype(BF16)
    return (own + up.astype(F32) + down.astype(F32)).astype(BF16)


def per_device(tokens, cotangent, gate_weight, up_weight, down_weight):
    n_dp, n_mp = lax.axis_size("dp"), lax.axis_size("mp")
    bits = n_dp.bit_length() - 1
    assert 1 << bits == n_dp and bits >= 1
    index = lax.axis_index("dp")
    width = tokens.shape[1]

    def assemble(x):
        blocks = gather_mp(localize(x, bits, index), n_mp)
        return jnp.stack([b.reshape(n_dp, -1, width) for b in blocks], axis=1).reshape(-1, width)

    def swap(x, step):
        return lax.ppermute(x, "dp", partners(n_dp, bits, step))

    def reduce_dp(rows, dot):
        half = rows.shape[0] // 2
        sent = dot(rows[half:]).astype(BF16)
        got = swap(sent, 0)
        kept = lax.optimization_barrier(dot(rows[:half]))
        for step in range(1, bits):
            total = kept + got.astype(F32)
            half = half // 2
            got = swap(total[half:].astype(BF16), step)
            kept = total[:half]
        return kept + got.astype(F32), sent

    def gather_dp(x):
        for step in range(bits - 1, -1, -1):
            x = jnp.concatenate([x, swap(x, step)])
        return x

    def finish(partial):
        partial = partial.astype(BF16).reshape(n_dp, n_mp, -1, width)
        blocks = [partial[:, k].reshape(-1, width) for k in range(n_mp)]
        return localize(scatter_mp(blocks, n_mp), bits, index, inverse=True)

    all_tokens = assemble(tokens)
    gate, sent = reduce_dp(all_tokens, lambda r: contract(r, gate_weight, 1, 0))
    up, _ = reduce_dp(all_tokens, lambda r: contract(r, up_weight, 1, 0))
    late, _ = lax.optimization_barrier((cotangent, sent))
    all_cotangent = assemble(late)
    d_hidden, _ = reduce_dp(all_cotangent, lambda r: contract(r, down_weight, 1, 1))
    sig = jax.nn.sigmoid(gate)
    hidden = (gate * sig * up).astype(BF16)
    all_hidden = gather_dp(hidden)
    d_gate = (d_hidden * up * sig * (1.0 + gate * (1.0 - sig))).astype(BF16)
    d_up = (d_hidden * gate * sig).astype(BF16)
    all_d_gate, all_d_up = gather_dp(d_gate), gather_dp(d_up)

    output = finish(contract(all_hidden, down_weight, 1, 0))
    grad_input = finish(
        contract(all_d_gate, gate_weight, 1, 1) + contract(all_d_up, up_weight, 1, 1)
    )
    turned = all_tokens.T
    grad_down = contract(all_hidden, all_cotangent, 0, 0).astype(BF16)
    grad_gate = contract(turned, all_d_gate, 1, 0).astype(BF16)
    grad_up = contract(turned, all_d_up, 1, 0).astype(BF16)
    return (output, grad_input, grad_gate, grad_up, grad_down)


def solution(mesh):
    placed = (P("mp", "dp"), P("mp", "dp"), P("dp", "mp"), P("dp", "mp"), P("mp", "dp"))
    return jax.shard_map(
        per_device,
        mesh=mesh,
        in_specs=placed,
        out_specs=(P("mp", "dp"), P("mp", "dp"), P("dp", "mp"), P("dp", "mp"), P("mp", "dp")),
        check_vma=False,
    )
```
